128 devices in a mesh: ep: 8 (over x, core), fsdp: 16 (over z, y).
Axes of the slice: x: 4, y: 4, z: 4, core: 2. Of those that a mesh axis runs over, the one named last changes fastest.
Arguments:
- master_gate: float32 [128, 2048, 768], P('ep', 'fsdp'), may hold values from -0.1875 to 0.1875
- master_up: float32 [128, 2048, 768], P('ep', 'fsdp'), may hold values from -0.1875 to 0.1875
- router_weight: float32 [2048, 128], P('fsdp', 'ep'), may hold values from -0.125 to 0.125
- router_gain: float32 [2048], P('fsdp'), may hold values from 0.25 to 1.75
Outputs:
- final_gate: bfloat16 [128, 2048, 768], P(('ep', 'fsdp'))
- final_up: bfloat16 [128, 2048, 768], P(('ep', 'fsdp'))
- scale_gate: float32 [128, 768], P(('ep', 'fsdp'))
- scale_up: float32 [128, 768], P(('ep', 'fsdp'))
- serve_router: bfloat16 [2048, 128], replicated
The draws below stay inside these ranges and needn't reach their ends.
All inputs are finite; a program needn't handle non-finite values.
Results may differ from the reference program's by a relative error of at most 0.001.
Values may be sent and summed in bfloat16 or wider, within the bound.
No kernel may reach another device: no remote copies, remote signals or barrier semaphores. Data moves between devices by JAX's collectives and lax.ppermute only.
A program may use at most 128 MiB of HBM per device.

```python
import jax
import jax.numpy as jnp
from jax import lax

EXPERTS = 128
D_MODEL = 2048
D_EXPERT = 768


def with_spikes(drawn, own_key, source, target, blocks, factor):
    owner, partner = [(jnp.arange(drawn.shape[axis_at]) // (drawn.shape[axis_at] // blocks)).reshape([-1 if axis == axis_at else 1 for axis in range(drawn.ndim)]) for axis_at in (source, target)]
    chosen = jax.random.permutation(own_key, blocks)[partner]
    strong = (owner == chosen) | (owner == (partner + blocks // 2) % blocks)
    return jnp.where(strong, factor * drawn, drawn)


def level_of(stream_key, dims, pieces, least, high):
    loudness = 1.0
    for dim, parts in pieces:
        heights = jax.random.uniform(jax.random.fold_in(jax.random.fold_in(stream_key, 6), dim), (parts,), jnp.float32, least / len(pieces), high / len(pieces))
        loudness = loudness * jnp.repeat(jnp.exp(heights), dims[dim] // parts).reshape((-1,) + (1,) * (len(dims) - 1 - dim))
    return loudness


def noise(rng, shape, scale, limit, pieces=(), kind=jnp.bfloat16):
    result = scale * jax.random.normal(rng, shape, jnp.float32)
    if pieces:
        result = result * level_of(rng, shape, pieces, -0.22, 0.18)
    return jnp.clip(result, -limit, limit).astype(kind)


def gaussian_with(stream_key, extent, spread, most, cuts, heavy, kind=jnp.bfloat16):
    result = spread * jax.random.normal(stream_key, extent, jnp.float32)
    if cuts:
        result = result * level_of(stream_key, extent, cuts, -0.22, 0.18)
    return jnp.clip(with_spikes(result, jax.random.fold_in(stream_key, 3), *heavy), -most, most).astype(kind)


def setup_inputs(seed: int = 0) -> dict:
    streams_of = jax.random.split(jax.random.key(seed), 5)
    return {
        "master_gate": gaussian_with(streams_of[0], (EXPERTS, D_MODEL, D_EXPERT), D_MODEL ** -0.5, 0.1875, ((0, 8), (1, 16)), (1, 2, 16, 2.0), jnp.float32),
        "master_up": gaussian_with(streams_of[1], (EXPERTS, D_MODEL, D_EXPERT), D_MODEL ** -0.5, 0.1875, ((0, 8), (1, 16)), (1, 2, 16, 2.0), jnp.float32),
        "router_weight": noise(streams_of[2], (D_MODEL, EXPERTS), D_MODEL ** -0.5, 0.125, ((0, 16), (1, 8)), jnp.float32),
        "router_gain": jnp.clip(1.0 + 0.15 * jax.random.normal(streams_of[3], (D_MODEL,), jnp.float32), 0.25, 1.75),
    }


def reference(master_gate, master_up, router_weight, router_gain):
    scale_gate = jnp.sqrt(lax.optimization_barrier(jnp.sum(master_gate * master_gate, axis=1)))
    final_gate = (master_gate / jnp.expand_dims(scale_gate, 1)).astype(jnp.bfloat16)
    scale_up = jnp.sqrt(lax.optimization_barrier(jnp.sum(master_up * master_up, axis=1)))
    final_up = (master_up / jnp.expand_dims(scale_up, 1)).astype(jnp.bfloat16)
    serve_router = (router_weight * router_gain[:, None]).astype(jnp.bfloat16)
    return (final_gate, final_up, scale_gate, scale_up, serve_router)
```

```python
import functools

import jax
import jax.numpy as jnp
from jax import lax
from jax.experimental import pallas as pl
from jax.experimental.pallas import tpu as pltpu
from jax.sharding import Mesh
from jax.sharding import PartitionSpec as P

EP = ("ep_0", "ep_1")
ALL = ("ep_0", "ep_1", "z", "y")
SIDE = 4
ORDER = (1, 3, 2)


def moved(value, axis, step):
    return lax.ppermute(value, axis, [(i, (i + step) % SIDE) for i in range(SIDE)])


def place(axis, step):
    return lax.bitwise_and(lax.axis_index(axis) + step + SIDE, SIDE - 1)


def summed(value, axis):
    parts = [moved(value, axis, k) for k in ORDER]
    return value + parts[0] + parts[1] + parts[2]


def at(value, axis, k):
    return lax.dynamic_index_in_dim(value, k, axis, keepdims=False)


def scaled(master, scale, axis, k):
    return (at(master, axis, k) / at(scale, axis, k)[:, None, :]).astype(jnp.bfloat16)


def joined(blocks):
    return jnp.stack(blocks)


def two_stages(master, scale, first, second):
    one = 1 if first == "y" else 0
    own = scaled(master, scale, one, place(first, 0))
    near = {k: moved(scaled(master, scale, one, place(first, k)), first, k) for k in ORDER}
    here = {0: own, **near}
    out = jnp.zeros(master.shape, jnp.bfloat16)

    def put(out, block, d_first, d_second):
        f, s = place(first, -d_first), place(second, -d_second)
        spot = (s, f) if one == 1 else (f, s)
        return lax.dynamic_update_slice(out, block[None, None], (*spot, 0, 0))

    sent = {}
    for d in ORDER:
        a = joined([at(here[k], 0, place(second, d)) for k in (0, 1, 3)])
        sent[d] = moved(a, second, d)
    last = {}
    for d in ORDER:
        last[d] = moved(at(here[2], 0, place(second, d)), second, d)
    for k in (0, 1, 3, 2):
        out = put(out, at(here[k], 0, place(second, 0)), k, 0)
    for d in ORDER:
        for i, k in enumerate((0, 1, 3)):
            out = put(out, sent[d][i], k, d)
    for d in ORDER:
        out = put(out, last[d], 2, d)
    return out


def router(weight, gain):
    part = (weight * gain[:, None]).astype(jnp.bfloat16)
    devices = SIDE * SIDE
    rows = lax.all_to_all(
        jnp.broadcast_to(part[None], (devices, *part.shape)), ("z", "y"), 0, 0, tiled=True
    ).reshape(1, -1, part.shape[1])
    some = lax.all_gather(rows, "ep_0", axis=0, tiled=True)
    every = lax.all_gather(some, "ep_1", axis=0, tiled=True)
    every = every.reshape(2, SIDE, *rows.shape[1:])
    return every.transpose(2, 1, 0, 3).reshape(rows.shape[1], -1)


def body(master_gate, master_up, router_weight, router_gain):
    _, rows, columns = master_gate.shape
    total = jnp.stack(
        [jnp.sum(master_gate * master_gate, axis=1), jnp.sum(master_up * master_up, axis=1)]
    )
    scale = jnp.sqrt(summed(summed(total, "y"), "z"))
    fours = scale.reshape(2, SIDE, SIDE, columns)
    whole = (SIDE, SIDE, rows, columns)
    gate = two_stages(master_gate.reshape(whole), fours[0], "y", "z")
    up = two_stages(master_up.reshape(whole), fours[1], "z", "y")
    mine = lax.dynamic_slice(
        fours, (0, place("z", 0), place("y", 0), 0), (2, 1, 1, columns)
    ).reshape(2, columns)
    serve = router(router_weight, router_gain)
    flat = (1, SIDE * SIDE * rows, columns)
    return gate.reshape(flat), up.reshape(flat), mine[0:1], mine[1:2], serve


def solution(mesh):
    finer = Mesh(mesh.devices.reshape(4, 2, SIDE, SIDE), ALL)
    fsdp = ("z", "y")
    return jax.shard_map(
        body,
        mesh=finer,
        in_specs=(P(EP, fsdp, None), P(EP, fsdp, None), P(fsdp, EP), P(fsdp)),
        out_specs=(P(ALL, None, None), P(ALL, None, None), P(ALL, None), P(ALL, None), P()),
        check_vma=False,
    )
```

```python
import functools

import jax
import jax.numpy as jnp
from jax import lax
from jax.experimental import pallas as pl
from jax.experimental.pallas import tpu as pltpu
from jax.sharding import Mesh
from jax.sharding import PartitionSpec as P

EP = ("x", "core")
ALL = ("x", "core", "z", "y")
SIDE = 4
LANES = 128
STEPS = (1, 3, 2)
WITH_OWN = (0, 1, 3, 2)
VMEM = pl.BlockSpec(memory_space=pltpu.VMEM)
HBM = pl.BlockSpec(memory_space=pltpu.HBM)
f32, bf16 = jnp.float32, jnp.bfloat16


def moved(value, axis, step):
    return lax.ppermute(value, axis, [(i, (i + step) % SIDE) for i in range(SIDE)])


def place(axis, step=0):
    return lax.bitwise_and(lax.axis_index(axis) + (step + SIDE), SIDE - 1)


def rows_at(start, size):
    return pl.ds(pl.multiple_of(start, 8), size)


def cost(nbytes, flops=0):
    return pl.CostEstimate(flops=max(flops, nbytes), bytes_accessed=nbytes, transcendentals=0)


def limit(mib):
    return pltpu.CompilerParams(vmem_limit_bytes=mib << 20)


def sums_kernel(master, out):
    experts, _, columns = master.shape
    tiles = columns // LANES

    def one(e, carry):
        for j in range(tiles):
            x = master[e, :, j * LANES : (j + 1) * LANES]
            out[pl.ds(j * experts + e, 1), :] = jnp.sum(x * x, axis=0, keepdims=True)
        return carry

    lax.fori_loop(0, experts, one, 0)


def last_sums_kernel(master, other, weight, gain, out, held):
    sums_kernel(master, held)
    n = other.shape[0]
    out[pl.ds(0, n), :] = other[...]
    out[pl.ds(n, n), :] = held[...]
    out[pl.ds(2 * n, weight.shape[0]), :] = (weight[...] * gain[...]).astype(bf16).astype(f32)


def sums(gate, up, weight, gain):
    experts, _, columns = gate.shape
    n = experts * columns // LANES
    one = pl.pallas_call(
        sums_kernel,
        in_specs=[VMEM],
        out_specs=VMEM,
        out_shape=jax.ShapeDtypeStruct((n, LANES), f32),
        cost_estimate=cost(gate.size * 4),
        name="sums",
        compiler_params=limit(8),
    )(gate)
    return pl.pallas_call(
        last_sums_kernel,
        in_specs=[VMEM] * 4,
        out_specs=VMEM,
        out_shape=jax.ShapeDtypeStruct((2 * n + weight.shape[0], LANES), f32),
        scratch_shapes=[pltpu.VMEM((n, LANES), f32)],
        cost_estimate=cost(up.size * 4),
        name="last_sums",
        compiler_params=limit(8),
    )(up, one, weight, gain)


def along_y_kernel(n, own, r1, r3, r2, out):
    out[pl.ds(0, n), :] = (own[:n, :] + r1[:n, :]) + (r2[:n, :] + r3[:n, :])
    more = own.shape[0] - n
    for k, ref in zip(WITH_OWN, (own, r1, r3, r2)):
        out[rows_at(n + place("y", -k) * more, more), :] = ref[n:, :]


def along_z_kernel(n, experts, own, r1, r3, r2, inverse, mine_gate, mine_up, router, scale):
    scale[...] = jnp.sqrt((own[:n, :] + r1[:n, :]) + (r2[:n, :] + r3[:n, :]))
    inverse[...] = 1.0 / scale[...]
    e = place("z") * SIDE + place("y")
    tiles = n // (2 * experts)
    for a, mine in enumerate((mine_gate, mine_up)):
        for j in range(tiles):
            mine[:, j * LANES : (j + 1) * LANES] = scale[pl.ds((a * tiles + j) * experts + e, 1), :]
    columns = router.shape[0]
    for k, ref in zip(WITH_OWN, (own, r1, r3, r2)):
        for y in range(SIDE):
            lane = (place("z", -k) * SIDE + y) * LANES
            part = ref[n + y * columns : n + (y + 1) * columns, :]
            router[:, pl.ds(pl.multiple_of(lane, LANES), LANES)] = part.astype(bf16)


def exchange_of_sums(payload, n, experts, columns):
    height, more = payload.shape[0], payload.shape[0] - n
    parts = [moved(payload, "y", k) for k in STEPS]
    tall = n + SIDE * more
    both = pl.pallas_call(
        functools.partial(along_y_kernel, n),
        in_specs=[VMEM] * 4,
        out_specs=VMEM,
        out_shape=jax.ShapeDtypeStruct((tall, LANES), f32),
        cost_estimate=cost(4 * payload.size),
        name="along_y",
        compiler_params=limit(4),
    )(payload, *parts)
    parts = [moved(both, "z", k) for k in STEPS]
    return pl.pallas_call(
        functools.partial(along_z_kernel, n, experts),
        in_specs=[VMEM] * 4,
        out_specs=[VMEM] * 4,
        out_shape=[
            jax.ShapeDtypeStruct((n, LANES), f32),
            jax.ShapeDtypeStruct((1, columns), f32),
            jax.ShapeDtypeStruct((1, columns), f32),
            jax.ShapeDtypeStruct((more, SIDE * SIDE * LANES), bf16),
        ],
        scratch_shapes=[pltpu.VMEM((n, LANES), f32)],
        cost_estimate=cost(4 * both.size),
        name="along_z",
        compiler_params=limit(4),
    )(both, *parts)


def scale_kernel(first, plan, master, inverse, *outs):
    tiles = master.shape[-1] // LANES
    for i, (half, step) in enumerate(plan):

        def some(k, carry, i=i, half=half, step=step):
            z, y = (k, place("y", step)) if half == 0 else (place("z", step), k)
            for j in range(tiles):
                lanes = pl.ds(j * LANES, LANES)
                row = inverse[pl.ds((first + j) * SIDE * SIDE + z * SIDE + y, 1), :]
                outs[i][k, :, lanes] = (master[z, y, half, :, lanes] * row).astype(bf16)
            return carry

        lax.fori_loop(0, SIDE, some, 0)


def scaled(master, inverse, first, plan):
    rows, columns = master.shape[-2:]
    piece = (SIDE, rows, columns)
    size = len(plan) * SIDE * rows * columns
    outs = pl.pallas_call(
        functools.partial(scale_kernel, first, plan),
        in_specs=[VMEM, VMEM],
        out_specs=[VMEM] * len(plan),
        out_shape=[jax.ShapeDtypeStruct(piece, bf16)] * len(plan),
        cost_estimate=cost(6 * size),
        name="scaled",
        compiler_params=limit(16),
    )(master, inverse)
    return dict(zip(plan, outs))


def regroup_kernel(*refs):
    ins, outs = refs[: 2 * SIDE], refs[2 * SIDE :]
    for half, (one, two) in enumerate((("y", "z"), ("z", "y"))):
        for o, d in enumerate(STEPS):
            for i, k in enumerate(WITH_OWN):
                outs[half * len(STEPS) + o][place(one, -k)] = ins[half * SIDE + i][place(two, d)]


def regroup(parts):
    shape = parts[0].shape
    count = 2 * len(STEPS)
    return pl.pallas_call(
        regroup_kernel,
        in_specs=[VMEM] * len(parts),
        out_specs=[VMEM] * count,
        out_shape=[jax.ShapeDtypeStruct(shape, bf16)] * count,
        cost_estimate=cost(2 * count * parts[0].size * 2),
        name="regroup",
        compiler_params=limit(16),
    )(*parts)


def own_kernel(*refs):
    ins, (out, sems) = refs[: 2 * SIDE], refs[2 * SIDE :]
    copies = []
    for half in range(2):
        for i, k in enumerate(WITH_OWN):
            if half == 0:
                source, target = ins[i].at[place("z")], out.at[place("z"), place("y", -k), 0]
            else:
                source, target = ins[SIDE + i].at[place("y")], out.at[place("z", -k), place("y"), 1]
            copies.append(pltpu.make_async_copy(source, target, sems.at[half * SIDE + i]))
    for c in copies:
        c.start()
    for c in copies:
        c.wait()


def put_own(parts):
    _, rows, columns = parts[0].shape
    shape = (SIDE, SIDE, 2, rows, columns)
    return pl.pallas_call(
        own_kernel,
        in_specs=[VMEM] * len(parts),
        out_specs=HBM,
        out_shape=jax.ShapeDtypeStruct(shape, bf16),
        scratch_shapes=[pltpu.SemaphoreType.DMA((2 * SIDE,))],
        cost_estimate=cost(8 * parts[0].size),
        name="put_own",
        compiler_params=limit(16),
    )(*parts)


def put_kernel(_, *refs):
    ins, (out, sems) = refs[: 2 * len(STEPS)], refs[2 * len(STEPS) :]
    copies = []
    for half in range(2):
        for i, d in enumerate(STEPS):
            target = out.at[place("z", -d), :, 0] if half == 0 else out.at[:, place("y", -d), 1]
            n = half * len(STEPS) + i
            copies.append(pltpu.make_async_copy(ins[n], target, sems.at[n]))
    for c in copies:
        c.start()
    for c in copies:
        c.wait()


def put(out, parts):
    return pl.pallas_call(
        put_kernel,
        in_specs=[HBM] + [VMEM] * len(parts),
        out_specs=HBM,
        out_shape=jax.ShapeDtypeStruct(out.shape, bf16),
        scratch_shapes=[pltpu.SemaphoreType.DMA((len(parts),))],
        input_output_aliases={0: 0},
        cost_estimate=cost(4 * len(parts) * parts[0].size),
        name="put",
        compiler_params=limit(16),
    )(out, *parts)


def stage_one(pieces):
    parts = {}
    for d in STEPS:
        for half, axis in ((0, "y"), (1, "z")):
            parts[half, d] = moved(pieces[half, d], axis, d)
    for half in range(2):
        parts[half, 0] = pieces[half, 0]
    return [parts[half, k] for half in range(2) for k in WITH_OWN]


def stage_two(parts):
    sent = regroup(parts)
    got = {}
    for i, d in enumerate(STEPS):
        for half, axis in ((0, "z"), (1, "y")):
            got[half, i] = moved(sent[half * len(STEPS) + i], axis, d)
    return [got[half, i] for half in range(2) for i in range(len(STEPS))]


def pair_kernel(own, other, out):
    height = own.shape[0]
    core = lax.axis_index("core")
    out[rows_at(core * height, height), :] = own[...]
    out[rows_at((1 - core) * height, height), :] = other[...]


def turn_kernel(own, r1, r3, r2, out, held):
    height = own.shape[0]
    for k, ref in zip(WITH_OWN, (own, r1, r3, r2)):
        held[rows_at(place("x", -k) * height, height), :] = ref[...].astype(f32)
    for i in range(out.shape[0] // LANES):
        at = slice(i * LANES, (i + 1) * LANES)
        out[at, :] = held[:, at].T.astype(bf16)


def router(part):
    columns, rows = part.shape
    other = lax.ppermute(part, "core", [(0, 1), (1, 0)])
    two = pl.pallas_call(
        pair_kernel,
        in_specs=[VMEM] * 2,
        out_specs=VMEM,
        out_shape=jax.ShapeDtypeStruct((2 * columns, rows), bf16),
        cost_estimate=cost(8 * part.size),
        name="pair",
        compiler_params=limit(4),
    )(part, other)
    parts = [moved(two, "x", k) for k in STEPS]
    total = 2 * SIDE * columns
    return pl.pallas_call(
        turn_kernel,
        in_specs=[VMEM] * 4,
        out_specs=VMEM,
        out_shape=jax.ShapeDtypeStruct((rows, total), bf16),
        scratch_shapes=[pltpu.VMEM((total, rows), f32)],
        cost_estimate=cost(4 * rows * total),
        name="turn",
        compiler_params=limit(6),
    )(two, *parts)


def body(master_gate, master_up, router_weight, router_gain):
    experts, rows, columns = master_gate.shape
    n = 2 * experts * columns // LANES
    payload = sums(master_gate, master_up, router_weight.T, router_gain[None])
    inverse, mine_gate, mine_up, part = exchange_of_sums(payload, n, experts, columns)
    halves = (SIDE, SIDE, 2, rows // 2, columns)
    gate, up = master_gate.reshape(halves), master_up.reshape(halves)

    early = ((0, 1), (1, 1))
    late = ((0, 3), (1, 3), (0, 2), (1, 2), (0, 0), (1, 0))
    tiles = columns // LANES
    pieces = {**scaled(gate, inverse, 0, early), **scaled(gate, inverse, 0, late)}
    gate_parts = stage_one(pieces)
    up_parts = stage_one(scaled(up, inverse, tiles, early + late))
    part, up_parts[0] = lax.optimization_barrier((part, up_parts[0]))
    serve = router(part)
    gate_got = stage_two(gate_parts)
    up_got = stage_two(up_parts)
    final_gate = put(put_own(gate_parts), gate_got)
    final_up = put(put_own(up_parts), up_got)
    flat = (1, experts * rows, columns)
    return final_gate.reshape(flat), final_up.reshape(flat), mine_gate, mine_up, serve


def solution(mesh):
    finer = Mesh(mesh.devices.reshape(4, 2, SIDE, SIDE), ALL)
    fsdp = ("z", "y")
    return jax.shard_map(
        body,
        mesh=finer,
        in_specs=(P(EP, fsdp, None), P(EP, fsdp, None), P(fsdp, EP), P(fsdp)),
        out_specs=(P(ALL, None, None), P(ALL, None, None), P(ALL, None), P(ALL, None), P()),
        check_vma=False,
    )
```

```python
import functools

import jax
import jax.numpy as jnp
from jax import lax
from jax.experimental import pallas as pl
from jax.experimental.pallas import tpu as pltpu
from jax.sharding import Mesh
from jax.sharding import PartitionSpec as P

EP = ("x", "core")
ALL = ("x", "core", "z", "y")
SIDE = 4
LANES = 128
STEPS = (1, 3, 2)
WITH_OWN = (0, 1, 3, 2)
VMEM = pl.BlockSpec(memory_space=pltpu.VMEM)
HBM = pl.BlockSpec(memory_space=pltpu.HBM)
f32, bf16 = jnp.float32, jnp.bfloat16


def moved(value, axis, step):
    return lax.ppermute(value, axis, [(i, (i + step) % SIDE) for i in range(SIDE)])


def place(axis, step=0):
    return lax.bitwise_and(lax.axis_index(axis) + (step + SIDE), SIDE - 1)


def rows_at(start, size):
    return pl.ds(pl.multiple_of(start, 8), size)


def cost(nbytes, flops=0):
    return pl.CostEstimate(flops=max(flops, nbytes), bytes_accessed=nbytes, transcendentals=0)


def limit(mib):
    return pltpu.CompilerParams(vmem_limit_bytes=mib << 20)


def sums_kernel(master, out):
    sides, _, halves, _, columns = master.shape
    experts, tiles = sides * sides, columns // LANES

    def one(e, carry):
        z, y = lax.div(e, sides), lax.rem(e, sides)
        for j in range(tiles):
            total = 0.0
            for half in range(halves):
                x = master[z, y, half, :, j * LANES : (j + 1) * LANES]
                total += jnp.sum(x * x, axis=0, keepdims=True)
            out[pl.ds(j * experts + e, 1), :] = total
        return carry

    lax.fori_loop(0, experts, one, 0)


def first_sums_kernel(plan, master, out, *picked):
    for i, (half, step) in enumerate(plan):

        def some(k, carry, i=i, half=half, step=step):
            z, y = (k, place("y", step)) if half == 0 else (place("z", step), k)
            picked[i][k] = master[z, y, half]
            return carry

        lax.fori_loop(0, SIDE, some, 0)
    sums_kernel(master, out)


def last_sums_kernel(master, other, weight, gain, out, held):
    sums_kernel(master, held)
    n = other.shape[0]
    out[pl.ds(0, n), :] = other[...]
    out[pl.ds(n, n), :] = held[...]
    out[pl.ds(2 * n, weight.shape[0]), :] = (weight[...] * gain[...]).astype(bf16).astype(f32)


def first_sums(master, plan):
    rows, columns = master.shape[-2:]
    piece = (SIDE, rows, columns)
    n = SIDE * SIDE * columns // LANES
    one, *outs = pl.pallas_call(
        functools.partial(first_sums_kernel, plan),
        in_specs=[VMEM],
        out_specs=[VMEM] * (1 + len(plan)),
        out_shape=[jax.ShapeDtypeStruct((n, LANES), f32)]
        + [jax.ShapeDtypeStruct(piece, f32)] * len(plan),
        cost_estimate=cost(master.size * 4),
        name="first_sums",
        compiler_params=limit(12),
    )(master)
    return one, dict(zip(plan, outs))


def last_sums(master, one, weight, gain):
    n = one.shape[0]
    return pl.pallas_call(
        last_sums_kernel,
        in_specs=[VMEM] * 4,
        out_specs=VMEM,
        out_shape=jax.ShapeDtypeStruct((2 * n + weight.shape[0], LANES), f32),
        scratch_shapes=[pltpu.VMEM((n, LANES), f32)],
        cost_estimate=cost(master.size * 4),
        name="last_sums",
        compiler_params=limit(8),
    )(master, one, weight, gain)


def swapped(value, axis, kind):
    count = lax.axis_size(axis)
    other = (lambda i: i ^ 1) if kind == 0 else (lambda i: count - 1 - i)
    return lax.ppermute(value, axis, [(i, other(i)) for i in range(count)])


def bit(axis, kind):
    at = lax.axis_index(axis)
    return lax.bitwise_and(at, 1) if kind == 0 else lax.shift_right_logical(at, 1)


def join_kernel(n, axis, kind, own, other, *outs):
    more = own.shape[0] - n
    out = outs[0]
    if n:
        out[pl.ds(0, n), :] = own[:n, :] + other[:n, :]
    if more:
        rest, first = (outs[1], 0) if len(outs) > 1 else (out, n)
        mine = bit(axis, kind)
        rest[rows_at(first + mine * more, more), :] = own[n:, :].astype(rest.dtype)
        rest[rows_at(first + (1 - mine) * more, more), :] = other[n:, :].astype(rest.dtype)


def joined(own, axis, kind, n=0, apart=False):
    more = own.shape[0] - n
    if apart:
        shapes = [jax.ShapeDtypeStruct((n, LANES), f32), jax.ShapeDtypeStruct((2 * more, LANES), bf16)]
    else:
        shapes = [jax.ShapeDtypeStruct((n + 2 * more, LANES), own.dtype)]
    outs = pl.pallas_call(
        functools.partial(join_kernel, n, axis, kind),
        in_specs=[VMEM] * 2,
        out_specs=[VMEM] * len(shapes),
        out_shape=shapes,
        cost_estimate=cost(12 * own.size),
        name="joined",
        compiler_params=limit(4),
    )(own, swapped(own, axis, kind))
    return outs if apart else outs[0]


def roots_kernel(experts, own, other, inverse, mine_gate, mine_up, scale):
    n = own.shape[0]
    scale[...] = jnp.sqrt(own[...] + other[...])
    inverse[...] = 1.0 / scale[...]
    e = place("z") * SIDE + place("y")
    tiles = n // (2 * experts)
    for a, mine in enumerate((mine_gate, mine_up)):
        for j in range(tiles):
            mine[:, j * LANES : (j + 1) * LANES] = scale[pl.ds((a * tiles + j) * experts + e, 1), :]


def exchange_of_sums(payload, n, experts, columns):
    payload = joined(payload, "y", 0, n)
    payload, part = joined(payload, "y", 1, n, apart=True)
    payload = joined(payload, "z", 0, n)
    roots = pl.pallas_call(
        functools.partial(roots_kernel, experts),
        in_specs=[VMEM] * 2,
        out_specs=[VMEM] * 3,
        out_shape=[
            jax.ShapeDtypeStruct((n, LANES), f32),
            jax.ShapeDtypeStruct((1, columns), f32),
            jax.ShapeDtypeStruct((1, columns), f32),
        ],
        scratch_shapes=[pltpu.VMEM((n, LANES), f32)],
        cost_estimate=cost(4 * payload.size),
        name="roots",
        compiler_params=limit(4),
    )(payload, swapped(payload, "z", 1))
    return *roots, part


def scale_kernel(first, plan, master, inverse, *outs):
    tiles = master.shape[-1] // LANES
    for i, (half, step) in enumerate(plan):

        def some(k, carry, i=i, half=half, step=step):
            z, y = (k, place("y", step)) if half == 0 else (place("z", step), k)
            for j in range(tiles):
                lanes = pl.ds(j * LANES, LANES)
                row = inverse[pl.ds((first + j) * SIDE * SIDE + z * SIDE + y, 1), :]
                outs[i][k, :, lanes] = (master[z, y, half, :, lanes] * row).astype(bf16)
            return carry

        lax.fori_loop(0, SIDE, some, 0)


def scaled(master, inverse, first, plan):
    rows, columns = master.shape[-2:]
    piece = (SIDE, rows, columns)
    size = len(plan) * SIDE * rows * columns
    outs = pl.pallas_call(
        functools.partial(scale_kernel, first, plan),
        in_specs=[VMEM, VMEM],
        out_specs=[VMEM] * len(plan),
        out_shape=[jax.ShapeDtypeStruct(piece, bf16)] * len(plan),
        cost_estimate=cost(6 * size),
        name="scaled",
        compiler_params=limit(16),
    )(master, inverse)
    return dict(zip(plan, outs))


def regroup_kernel(first, *refs):
    ins, inverse, outs = refs[: 2 * SIDE], refs[2 * SIDE], refs[2 * SIDE + 1 :]
    tiles = ins[0].shape[-1] // LANES
    for half, (one, two) in enumerate((("y", "z"), ("z", "y"))):
        for i, k in enumerate(WITH_OWN):
            source = ins[half * SIDE + i]
            for o, d in enumerate(WITH_OWN):
                target, to = outs[half * SIDE + o], place(one, -k)
                if source.dtype == bf16:
                    target[to] = source[place(two, d)]
                    continue
                z, y = (place("z", d), place("y")) if half == 0 else (place("z"), place("y", d))
                for j in range(tiles):
                    lanes = pl.ds(j * LANES, LANES)
                    row = inverse[pl.ds((first + j) * SIDE * SIDE + z * SIDE + y, 1), :]
                    target[to, :, lanes] = (source[place(two, d), :, lanes] * row).astype(bf16)


def regroup(parts, inverse, first):
    shape = parts[0].shape
    return pl.pallas_call(
        functools.partial(regroup_kernel, first),
        in_specs=[VMEM] * (len(parts) + 1),
        out_specs=[VMEM] * len(parts),
        out_shape=[jax.ShapeDtypeStruct(shape, bf16)] * len(parts),
        cost_estimate=cost(4 * len(parts) * parts[0].size),
        name="regroup",
        compiler_params=limit(16),
    )(*parts, inverse)


def own_kernel(first, second, out, sems):
    copies = [
        pltpu.make_async_copy(first, out.at[place("z"), :, 0], sems.at[0]),
        pltpu.make_async_copy(second, out.at[:, place("y"), 1], sems.at[1]),
    ]
    for c in copies:
        c.start()
    for c in copies:
        c.wait()


def put_own(first, second):
    _, rows, columns = first.shape
    return pl.pallas_call(
        own_kernel,
        in_specs=[VMEM] * 2,
        out_specs=HBM,
        out_shape=jax.ShapeDtypeStruct((SIDE, SIDE, 2, rows, columns), bf16),
        scratch_shapes=[pltpu.SemaphoreType.DMA((2,))],
        cost_estimate=cost(8 * first.size),
        name="put_own",
        compiler_params=limit(16),
    )(first, second)


def put_kernel(_, *refs):
    ins, (out, sems) = refs[: 2 * len(STEPS)], refs[2 * len(STEPS) :]
    copies = []
    for half in range(2):
        for i, d in enumerate(STEPS):
            target = out.at[place("z", -d), :, 0] if half == 0 else out.at[:, place("y", -d), 1]
            n = half * len(STEPS) + i
            copies.append(pltpu.make_async_copy(ins[n], target, sems.at[n]))
    for c in copies:
        c.start()
    for c in copies:
        c.wait()


def put(out, parts):
    return pl.pallas_call(
        put_kernel,
        in_specs=[HBM] + [VMEM] * len(parts),
        out_specs=HBM,
        out_shape=jax.ShapeDtypeStruct(out.shape, bf16),
        scratch_shapes=[pltpu.SemaphoreType.DMA((len(parts),))],
        input_output_aliases={0: 0},
        cost_estimate=cost(4 * len(parts) * parts[0].size),
        name="put",
        compiler_params=limit(16),
    )(out, *parts)


def stage_two(grouped):
    got = {}
    for i, d in enumerate(STEPS):
        for half, axis in ((0, "z"), (1, "y")):
            got[half, i] = moved(grouped[half * SIDE + 1 + i], axis, d)
    return [got[half, i] for half in range(2) for i in range(len(STEPS))]


def turn_kernel(columns, own, other, out, held):
    half = own.shape[0]
    mine = bit("x", 1)
    held[rows_at(mine * half, half), :] = own[...].astype(f32)
    held[rows_at((1 - mine) * half, half), :] = other[...].astype(f32)
    sources = SIDE * SIDE
    groups = 2 * half // (sources * columns)
    for s in range(sources):
        parts = [held[pl.ds((g * sources + s) * columns, columns), :] for g in range(groups)]
        out[s * LANES : (s + 1) * LANES, :] = jnp.concatenate(parts, axis=0).T.astype(bf16)


def turned(own, other, columns):
    return pl.pallas_call(
        functools.partial(turn_kernel, columns),
        in_specs=[VMEM] * 2,
        out_specs=VMEM,
        out_shape=jax.ShapeDtypeStruct((SIDE * SIDE * LANES, LANES), bf16),
        scratch_shapes=[pltpu.VMEM((2 * own.shape[0], LANES), f32)],
        cost_estimate=cost(16 * own.size),
        name="turned",
        compiler_params=limit(6),
    )(own, other)


def body(master_gate, master_up, router_weight, router_gain):
    experts, rows, columns = master_gate.shape
    n = 2 * experts * columns // LANES
    tiles = columns // LANES
    halves = (SIDE, SIDE, 2, rows // 2, columns)
    gate, up = master_gate.reshape(halves), master_up.reshape(halves)
    axes = ("y", "z")
    near = [(half, d) for d in (1, 3) for half in range(2)]
    far = [(half, 2) for half in range(2)]
    own = [(half, 0) for half in range(2)]

    one, early = first_sums(gate, near)
    gate_one = {(h, 1): moved(early[h, 1], axes[h], 1) for h in range(2)}
    payload = last_sums(up, one, router_weight.T, router_gain[None])
    payload, *held = lax.optimization_barrier((payload, *[early[h, 3] for h in range(2)]))
    gate_one |= {(h, 3): moved(held[h], axes[h], 3) for h in range(2)}
    inverse, mine_gate, mine_up, part = exchange_of_sums(payload, n, experts, columns)

    late = scaled(gate, inverse, 0, far + own)
    gate_one |= {(h, 2): moved(late[h, 2], axes[h], 2) for h in range(2)}
    gate_one |= {key: late[key] for key in own}
    pieces = scaled(up, inverse, tiles, near + far + own)
    up_one = {(h, d): moved(pieces[h, d], axes[h], d) for h, d in near}
    part, pieces[0, 0] = lax.optimization_barrier((part, pieces[0, 0]))
    part = joined(part, "z", 0)
    part, *held = lax.optimization_barrier((part, *[pieces[key] for key in far]))
    up_one |= {(h, 2): moved(held[h], axes[h], 2) for h in range(2)}
    up_one |= {key: pieces[key] for key in own}

    part = joined(joined(part, "z", 1), "core", 0)
    ordered = [(h, k) for h in range(2) for k in WITH_OWN]
    gate_parts = [gate_one[key] for key in ordered]
    part, gate_parts[0] = lax.optimization_barrier((part, gate_parts[0]))
    gate_grouped = regroup(gate_parts, inverse, 0)
    gate_got = stage_two(gate_grouped)

    part = joined(part, "x", 0)
    up_parts = [up_one[key] for key in ordered]
    part, up_parts[0] = lax.optimization_barrier((part, up_parts[0]))
    up_grouped = regroup(up_parts, inverse, tiles)
    up_got = stage_two(up_grouped)
    final_gate = put(put_own(gate_grouped[0], gate_grouped[SIDE]), gate_got)
    final_up = put(put_own(up_grouped[0], up_grouped[SIDE]), up_got)
    serve = turned(part, swapped(part, "x", 1), router_weight.shape[1])
    flat = (1, experts * rows, columns)
    return final_gate.reshape(flat), final_up.reshape(flat), mine_gate, mine_up, serve


def solution(mesh):
    finer = Mesh(mesh.devices.reshape(4, 2, SIDE, SIDE), ALL)
    fsdp = ("z", "y")
    return jax.shard_map(
        body,
        mesh=finer,
        in_specs=(P(EP, fsdp, None), P(EP, fsdp, None), P(fsdp, EP), P(fsdp)),
        out_specs=(P(ALL, None, None), P(ALL, None, None), P(ALL, None), P(ALL, None), P()),
        check_vma=False,
    )
```
